32 devices in a mesh: cols: 8 (over z, x), rows: 4 (over y, core).
Axes of the slice: x: 2, y: 2, z: 4, core: 2. Of those that a mesh axis runs over, the one named last changes fastest.
Arguments:
- vectors: float32 [8192, 4096], P('rows', 'cols'), may hold values from -6 to 6
- reflectors: float32 [4, 256, 8192], P(None, 'cols', 'rows'), may hold values from -0.0625 to 0.0625
- wy_factor: float32 [4, 256, 256], replicated, may hold values from -1 to 2, as said below
Outputs:
- transformed: float32 [8192, 4096], P('rows', 'cols')
The draws below stay inside these ranges and needn't reach their ends.
Inputs may be any that keep to these rules, and one draw needn't show every extreme that they name: Each wy_factor[k] is upper triangular with diagonal entries between 0.5 and 2.
All inputs are finite; a program needn't handle non-finite values.
Results may differ from the reference program's by a relative error of at most 0.00012.
Values sent between devices are 32-bit elements; how exact they have to be, the bound alone decides.
No kernel may reach another device: no remote copies, remote signals or barrier semaphores. Data moves between devices by JAX's collectives and lax.ppermute only.
A program may use at most 64 MiB of HBM per device.

```python
import jax
import jax.numpy as jnp
from jax import lax

NB = 256
PANELS = 4
M = 8192
NCOL = 4096


def draw_wy_factor(key, part):
    key_diag = jax.random.fold_in(key, 11)
    key_off = jax.random.fold_in(key, 12)
    diag = jax.random.uniform(key_diag, (PANELS, NB), jnp.float32, 0.8, 1.6)
    off = jnp.clip(0.03 * jax.random.normal(key_off, (PANELS, NB, NB), jnp.float32), -0.9, 0.9)
    upper = jnp.triu(off, 1)
    eye = jnp.eye(NB, dtype=jnp.float32)
    return upper + eye[None, :, :] * diag[:, :, None]


def level_of(own_key, shape, pieces, smallest, top_value):
    factor_of = 1.0
    for dim, parts in pieces:
        heights = jax.random.uniform(jax.random.fold_in(jax.random.fold_in(own_key, 6), dim), (parts,), jnp.float32, smallest / len(pieces), top_value / len(pieces))
        factor_of = factor_of * jnp.repeat(jnp.exp(heights), shape[dim] // parts).reshape((-1,) + (1,) * (len(shape) - 1 - dim))
    return factor_of


def scatter_about(key, dims, scale, bound, split=(), held_as=jnp.bfloat16):
    factor_of = level_of(key, dims, split, -0.22, 0.18) if split else 1.0
    result = jax.random.normal(key, dims, jnp.float32) * scale * factor_of
    return jnp.minimum(jnp.maximum(result, -bound), bound).astype(held_as)


def setup_inputs(seed: int = 0) -> dict:
    key_of = jax.random.split(jax.random.key(seed), 4)
    vectors = scatter_about(key_of[0], (M, NCOL), 1.0, 6.0, ((0, 4), (1, 8)), jnp.float32)
    reflectors = scatter_about(key_of[1], (PANELS, NB, M), M ** -0.5, 0.0625, ((1, 8), (2, 4)), jnp.float32)
    wy_factor = draw_wy_factor(jax.random.fold_in(key_of[3], 71), 0)
    return dict(vectors=vectors, reflectors=reflectors, wy_factor=wy_factor)


def reference(vectors, reflectors, wy_factor):
    current = vectors
    for panel in range(PANELS):
        basis = reflectors[panel]
        projection = jnp.dot(basis, current, precision=lax.Precision.HIGHEST, preferred_element_type=jnp.float32)
        scaled = jnp.dot(wy_factor[panel], projection, precision=lax.Precision.HIGHEST, preferred_element_type=jnp.float32)
        current = current - jnp.dot(basis.T, scaled, precision=lax.Precision.HIGHEST, preferred_element_type=jnp.float32)
    return current
```

```python
import jax
import jax.numpy as jnp
from jax import lax
from jax.sharding import PartitionSpec as P


RING = 8
WINDOW = 2

HOPS = (
    (0, 1), (1, 1), (0, 2), (1, 2), (0, 3), (2, 1), (0, 4), (1, 3),
    (2, 2), (1, 4), (3, 1), (2, 3), (2, 4), (3, 2), (3, 3), (3, 4),
)


def matmul(left, right, precision=lax.Precision.HIGH):
    return jnp.dot(left, right, precision=precision, preferred_element_type=jnp.float32)


def matmul_left_t(left, right):
    return lax.dot_general(
        left,
        right,
        (((0,), (0,)), ((), ())),
        precision=lax.Precision.HIGH,
        preferred_element_type=jnp.float32,
    )


def ring_order(n):
    return [c for c in range(n) if c % 2 == 0] + [c for c in reversed(range(n)) if c % 2 == 1]


def hop_order(panels, hops):
    if panels == 4 and hops == 4:
        return HOPS
    return tuple((k, s) for k in range(panels) for s in range(1, hops + 1))


def gather_panels(blocks, forward, backward, ring):
    hops = ring // 2
    half = blocks[0].shape[0] // 2
    ways = []
    for pairs, last in ((forward, slice(0, half)), (backward, slice(half, None))):
        held = {(k, 0): block for k, block in enumerate(blocks)}
        arrived = []
        for k, s in hop_order(len(blocks), hops):
            piece = held[k, s - 1]
            if s == hops:
                piece = piece[last]
            if len(arrived) >= WINDOW:
                piece, _ = lax.optimization_barrier((piece, arrived[-WINDOW]))
            held[k, s] = lax.ppermute(piece, "cols", pairs)
            arrived.append(held[k, s])
        ways.append(held)
    ahead, behind = ways
    return [
        jnp.concatenate(
            [ahead[k, s] for s in range(hops + 1)] + [behind[k, s] for s in range(hops, 0, -1)], axis=0
        )
        for k in range(len(blocks))
    ]


def rotated_factor(factor, order, place_of):
    ring = len(order)
    width = factor.shape[1]
    size = width // ring
    spot = (place_of - lax.iota(jnp.int32, width) // size) % ring
    owner = jnp.where(spot < ring // 2, 2 * spot, 2 * (ring - 1 - spot) + 1)
    wanted = owner * size + lax.iota(jnp.int32, width) % size
    pick = (wanted[:, None] == lax.iota(jnp.int32, width)[None, :]).astype(jnp.float32)
    rows = jnp.einsum("ij,kjl->kil", pick, factor, precision=lax.Precision.HIGHEST)
    return jnp.einsum("kil,jl->kij", rows, pick, precision=lax.Precision.HIGHEST)


def factored_sum(partial, factor, rows):
    if rows != 4:
        return matmul(factor, lax.psum(partial, "rows"), lax.Precision.HIGHEST)
    near = [(r, r ^ 1) for r in range(rows)]
    far = [(r, r ^ 2) for r in range(rows)]
    half = partial.shape[1] // 2
    second = lax.axis_index("rows") % 2 == 1
    left, right = partial[:, :half], partial[:, half:]
    keep = jnp.where(second, right, left)
    give = jnp.where(second, left, right)
    chip = keep + lax.ppermute(give, "rows", near)
    total = chip + lax.ppermute(chip, "rows", far)
    mine = matmul(factor, total, lax.Precision.HIGHEST)
    other = lax.ppermute(mine, "rows", near)
    return jnp.concatenate([jnp.where(second, other, mine), jnp.where(second, mine, other)], axis=1)


def solution(mesh):
    n, rows = mesh.shape["cols"], mesh.shape["rows"]
    ring = min(RING, n)
    inner = n // ring
    order = ring_order(ring)
    forward = [
        (order[i] * inner + j, order[(i + 1) % ring] * inner + j) for i in range(ring) for j in range(inner)
    ]
    backward = [(b, a) for a, b in forward]

    def per_device(vectors, reflectors, wy_factor):
        seat = lax.axis_index("cols") // inner
        place = jnp.where(seat % 2 == 0, seat // 2, ring - 1 - seat // 2)
        factor = rotated_factor(wy_factor, order, place)
        blocks = [reflectors[k] for k in range(reflectors.shape[0])]
        if inner > 1:
            groups = [list(range(q * inner, (q + 1) * inner)) for q in range(ring)]
            blocks = [
                lax.all_gather(block, "cols", axis=0, tiled=True, axis_index_groups=groups) for block in blocks
            ]
        current = vectors
        for k, basis in enumerate(gather_panels(blocks, forward, backward, ring)):
            scaled = factored_sum(matmul(basis, current), factor[k], rows)
            current = current - matmul_left_t(basis, scaled)
        return current

    return jax.shard_map(
        per_device,
        mesh=mesh,
        in_specs=(P("rows", "cols"), P(None, "cols", "rows"), P()),
        out_specs=P("rows", "cols"),
        check_vma=False,
    )
```
